32 devices in a mesh: gx: 8 (over z, y), gy: 4 (over x, core).
Axes of the slice: x: 2, y: 2, z: 4, core: 2. Of those that a mesh axis runs over, the one named last changes fastest.
Arguments:
- forces: float32 [3, 128, 128, 256], P(None, 'gx', 'gy'), may hold values from -8 to 8
- pressure_prev: float32 [128, 128, 256], P('gx', 'gy'), may hold values from -8 to 8
Outputs:
- pressure: float32 [128, 128, 256], P('gx', 'gy')
- residual: float32 [128, 128, 256], P('gx', 'gy')
The draws below stay inside these ranges and needn't reach their ends.
All inputs are finite; a program needn't handle non-finite values.
Results may differ from the reference program's by a relative error of at most 0.0003.
Values sent between devices are 32-bit elements; how exact they have to be, the bound alone decides.
A program may use at most 64 MiB of HBM per device.

```python
import jax
import jax.numpy as jnp
from jax import lax

NZ = 256
LEVELS = 5
SWEEPS = 2
COARSE_SWEEPS = 4
CYCLES = 2
NX = 128
NY = 128


def draw_pressure_prev(key, part):
    noise_key = jax.random.fold_in(key, 11)
    profile_key = jax.random.fold_in(key, 23)
    profile = 2.5 * jax.random.normal(profile_key, (NZ,), jnp.float32)
    noise = jax.random.normal(noise_key, (NX, NY, NZ), jnp.float32)
    return jnp.clip(noise + profile[None, None, :], -8.0, 8.0).astype(jnp.float32)


def block_scale(key, dims, shards, low, top_value):
    loudness, own = 1.0, jax.random.fold_in(key, 6)
    for dim, parts in shards:
        heights = jnp.exp(jax.random.uniform(jax.random.fold_in(own, dim), (parts,), jnp.float32, low / len(shards), top_value / len(shards)))
        loudness = loudness * jnp.repeat(heights, dims[dim] // parts).reshape([-1 if axis == dim else 1 for axis in range(len(dims))])
    return loudness


def normal_values(own_key, shape, spread, most, pieces=(), kind=jnp.bfloat16):
    gain = block_scale(own_key, shape, pieces, -0.22, 0.18) if pieces else 1.0
    drawn = jax.random.normal(own_key, shape, jnp.float32) * spread * gain
    return jnp.minimum(jnp.maximum(drawn, -most), most).astype(kind)


def setup_inputs(seed: int = 0) -> dict:
    splits = jax.random.split(jax.random.key(seed), 3)
    return {
        "forces": normal_values(splits[0], (3, NX, NY, NZ), 1.0, 8.0, ((1, 8), (2, 4)), jnp.float32),
        "pressure_prev": draw_pressure_prev(jax.random.fold_in(splits[2], 71), 0),
    }


OMEGA = 0.8

def vertical(values):
    padded = jnp.pad(values, ((0, 0), (0, 0), (1, 1)))
    return padded[:, :, 2:] + padded[:, :, :-2]

def operate_padded(padded, weight):
    center = padded[1:-1, 1:-1]
    beside = padded[2:, 1:-1] + padded[:-2, 1:-1] + padded[1:-1, 2:] + padded[1:-1, :-2]
    return weight * (4.0 * center - beside) + (2.0 * center - vertical(center))

def relax(padded, source, weight):
    center = padded[1:-1, 1:-1]
    return center + OMEGA * (source - operate_padded(padded, weight)) / (4.0 * weight + 2.0)

def wrapped(values):
    return jnp.pad(values, ((1, 1), (1, 1), (0, 0)), mode='wrap')

def restrict(residual_now):
    rows_x, rows_y, depth = residual_now.shape
    return 0.25 * residual_now.reshape(rows_x // 2, 2, rows_y // 2, 2, depth).sum(axis=(1, 3))

def prolong(correction):
    return jnp.repeat(jnp.repeat(correction, 2, axis=0), 2, axis=1)

def mean_mode(values, source):
    depth = source.shape[2]
    column = jnp.mean(source, axis=(0, 1))
    lower = jnp.concatenate([jnp.zeros((1,), source.dtype), -jnp.ones((depth - 1,), source.dtype)])
    upper = jnp.concatenate([-jnp.ones((depth - 1,), source.dtype), jnp.zeros((1,), source.dtype)])
    middle = 2.0 * jnp.ones((depth,), source.dtype)
    profile = lax.linalg.tridiagonal_solve(lower, middle, upper, column[:, None])[:, 0]
    return values + profile[None, None, :]

def whole_cycle(values, source, level_index):
    weight = 0.25 ** level_index
    if level_index == LEVELS - 1:
        values = mean_mode(values, source)
        for sweep_index in range(COARSE_SWEEPS):
            values = relax(wrapped(values), source, weight)
        return values
    for sweep_index in range(SWEEPS):
        values = relax(wrapped(values), source, weight)
    residual_now = source - operate_padded(wrapped(values), weight)
    coarse_source = restrict(residual_now)
    correction = whole_cycle(jnp.zeros_like(coarse_source), coarse_source, level_index + 1)
    values = values + prolong(correction)
    for sweep_index in range(SWEEPS):
        values = relax(wrapped(values), source, weight)
    return values

def reference(forces, pressure_prev):
    force_x, force_y, force_z = (forces[0], forces[1], forces[2])
    behind_x = jnp.roll(force_x, 1, axis=0)
    behind_y = jnp.roll(force_y, 1, axis=1)
    behind_z = jnp.pad(force_z[:, :, :-1], ((0, 0), (0, 0), (1, 0)))
    source = behind_x - force_x + (behind_y - force_y) + (behind_z - force_z)
    pressure = pressure_prev
    for cycle_index in range(CYCLES):
        pressure = whole_cycle(pressure, source, 0)
    residual = source - operate_padded(wrapped(pressure), 1.0)
    return (pressure, residual)
```

```python
import functools

import jax
import jax.numpy as jnp
from jax import lax
from jax.experimental import pallas as pl
from jax.experimental.pallas import tpu as pltpu
from jax.sharding import PartitionSpec as P

OMEGA = 0.8
PAD = 8
DIRS = [(dx, dy) for dx in (-1, 0, 1) for dy in (-1, 0, 1) if (dx, dy) != (0, 0)]
MESH = pl.DeviceIdType.MESH


def loop(count, body):
    def step(i, carry):
        body(i)
        return carry

    lax.fori_loop(0, count, step, 0)


def vertical(c):
    depth = c.shape[-1]
    axis = c.ndim - 1
    lane = lax.broadcasted_iota(jnp.int32, c.shape, axis)
    below = jnp.where(lane == 0, 0.0, pltpu.roll(c, 1, axis))
    above = jnp.where(lane == depth - 1, 0.0, pltpu.roll(c, depth - 1, axis))
    return below + above


def parts(ref, row, count):
    block = ref[pl.ds(row - 1, count + 2)]
    c = block[1:-1]
    width = c.shape[1]
    lateral = (block[:-2] + block[2:]) + (pltpu.roll(c, 1, 1) + pltpu.roll(c, width - 1, 1))
    return c, lateral, vertical(c)


def sweep(src, f, dst, row, rows, weight, unit, cols=None):
    k = OMEGA / (4.0 * weight + 2.0)

    def body(i):
        r = row + i * unit
        c, lateral, up = parts(src, r, unit)
        new = (1.0 - OMEGA) * c + k * (weight * lateral + up + f[pl.ds(r, unit)])
        if cols is None:
            dst[pl.ds(r, unit)] = new
        else:
            dst[pl.ds(r, unit), cols[0] : cols[1]] = new[:, cols[0] : cols[1]]

    loop(rows // unit, body)


def sweep_twice_from_zero(f, dst, row, rows, weight, unit):
    k = OMEGA / (4.0 * weight + 2.0)

    def body(i):
        r = row + i * unit
        c, lateral, up = parts(f, r, unit)
        dst[pl.ds(r, unit)] = k * ((2.0 - OMEGA) * c + k * (weight * lateral + up))

    loop(rows // unit, body)


def residual_rows(v, f, r, count, weight):
    c, lateral, up = parts(v, r, count)
    return f[pl.ds(r, count)] - ((4.0 * weight + 2.0) * c - weight * lateral - up)


def restricted(v, f, tmp, row, rows, cols, weight, put):
    start, count = cols
    depth = v.shape[-1]

    def body(i):
        r = residual_rows(v, f, row + 2 * i, 2, weight)
        both = r[0] + r[1]
        width = both.shape[0]
        halves = []
        for h in range(depth // 128):
            tmp[h, 0:width] = both[:, h * 128 : (h + 1) * 128]
            halves.append(
                tmp[h, pl.ds(start, count // 2, 2)] + tmp[h, pl.ds(start + 1, count // 2, 2)]
            )
        put(i, 0.25 * jnp.concatenate(halves, axis=1))

    loop(rows // 2, body)


def doubled(e, tmp, start):
    width, depth = e.shape
    for h in range(depth // 128):
        piece = e[:, h * 128 : (h + 1) * 128]
        tmp[h, pl.ds(start, width, 2)] = piece
        tmp[h, pl.ds(start + 1, width, 2)] = piece


def read_tmp(tmp, start, width):
    return jnp.concatenate([tmp[h, pl.ds(start, width)] for h in range(tmp.shape[0])], axis=1)


def ghosts(v, rows):
    v[0] = v[rows]
    v[rows + 1] = v[1]


def kernel(
    nx, ny, cycles,
    forces, pressure, out_p, out_r,
    fx, fy, fz, s, pa, pb, t0, t1, res,
    f1a, f1b, v1a, v1b, f2a, f2b, v2a, v2b, f3, v3a, v3b, f4, v4a, v4b, green, tmp,
    local_sem, plane_send, plane_recv, halo_send, halo_recv,
    g_send, g_recv, h_send, h_recv,
):
    mx, my = lax.axis_index("gx"), lax.axis_index("gy")
    n = nx * ny
    me = mx * ny + my
    bx, by, depth = pressure.shape
    cx1, cy1 = bx // 2, by // 2
    cx2, cy2 = bx // 4, by // 4

    loads = [
        pltpu.make_async_copy(forces.at[0], fx.at[pl.ds(1, bx)], local_sem.at[0]),
        pltpu.make_async_copy(forces.at[1], fy.at[:, pl.ds(PAD, by)], local_sem.at[1]),
        pltpu.make_async_copy(pressure, pa.at[pl.ds(PAD, bx), pl.ds(PAD, by)], local_sem.at[2]),
        pltpu.make_async_copy(forces.at[2], fz, local_sem.at[3]),
    ]
    for load in loads:
        load.start()

    barrier = pltpu.get_barrier_semaphore()

    def greet(j):
        other = lax.rem(me + 1 + j, n)
        pl.semaphore_signal(barrier, inc=1, device_id=(other // ny, lax.rem(other, ny)), device_id_type=MESH)

    loop(n - 1, greet)

    row_i = lax.broadcasted_iota(jnp.int32, (depth, depth), 0).astype(jnp.float32)
    col_i = lax.broadcasted_iota(jnp.int32, (depth, depth), 1).astype(jnp.float32)
    green[...] = (jnp.minimum(row_i, col_i) + 1.0) * (depth - jnp.maximum(row_i, col_i)) / (depth + 1.0)

    pl.semaphore_wait(barrier, n - 1)

    sends = []

    def halo(ref, size, width, slot):
        sx, sy = size
        copies = []
        for d, (dx, dy) in sorted(enumerate(DIRS), key=lambda e: abs(e[1][0]) * abs(e[1][1])):
            w = width - 1 if dx and dy else width
            if dx == 0:
                src_r, dst_r = pl.ds(PAD, sx), pl.ds(PAD, sx)
            elif dx == 1:
                src_r, dst_r = pl.ds(PAD + sx - w, w), pl.ds(PAD - w, w)
            else:
                src_r, dst_r = pl.ds(PAD, w), pl.ds(PAD + sx, w)
            if dy == 0:
                src_c, dst_c = pl.ds(PAD, sy), pl.ds(PAD, sy)
            elif dy == 1:
                src_c, dst_c = pl.ds(sy, PAD), pl.ds(0, PAD)
            else:
                src_c, dst_c = pl.ds(PAD, PAD), pl.ds(PAD + sy, PAD)
            copy = pltpu.make_async_remote_copy(
                src_ref=ref.at[src_r, src_c],
                dst_ref=ref.at[dst_r, dst_c],
                send_sem=halo_send.at[slot, d],
                recv_sem=halo_recv.at[slot, d],
                device_id=(lax.rem(mx + dx + nx, nx), lax.rem(my + dy + ny, ny)),
                device_id_type=MESH,
            )
            copy.start()
            copies.append(copy)
        sends.extend(copies)
        return copies

    def arrive(copies):
        for copy in copies:
            copy.wait_recv()

    right, above = lax.rem(mx + 1, nx), lax.rem(my + 1, ny)
    loads[0].wait()
    plane_x = pltpu.make_async_remote_copy(
        src_ref=fx.at[pl.ds(bx, 1)], dst_ref=fx.at[pl.ds(0, 1)],
        send_sem=plane_send.at[0], recv_sem=plane_recv.at[0],
        device_id=(right, my), device_id_type=MESH,
    )
    plane_x.start()
    loads[1].wait()
    plane_y = pltpu.make_async_remote_copy(
        src_ref=fy.at[:, pl.ds(by, PAD)], dst_ref=fy.at[:, pl.ds(0, PAD)],
        send_sem=plane_send.at[1], recv_sem=plane_recv.at[1],
        device_id=(mx, above), device_id_type=MESH,
    )
    plane_y.start()
    sends.extend([plane_x, plane_y])
    loads[2].wait()
    coming_p = halo(pa, (bx, by), 4, 0)
    loads[3].wait()
    plane_x.wait_recv()
    plane_y.wait_recv()

    def make_source(i):
        r = 2 * i
        x = fx[pl.ds(r, 3)]
        y = fy[pl.ds(r, 2)]
        z = fz[pl.ds(r, 2)]
        lane = lax.broadcasted_iota(jnp.int32, z.shape, 2)
        behind_z = jnp.where(lane == 0, 0.0, pltpu.roll(z, 1, 2))
        behind_y = pltpu.roll(y, 1, 1)[:, PAD:]
        s[pl.ds(PAD + r, 2), PAD : PAD + by] = (
            (x[:-1] - x[1:]) + (behind_y - y[:, PAD:]) + (behind_z - z)
        )

    loop(bx // 2, make_source)
    coming_s = halo(s, (bx, by), 4, 1)
    arrive(coming_p)
    arrive(coming_s)

    half = ny // 2
    many = nx * half
    parity = lax.rem(my, 2)
    partner = my + 1 - 2 * parity
    mine = mx * half + my // 2

    def solve_2(f2, turn):
        def place(x, y):
            return f2.at[pl.ds(1 + x * cx2, cx2), pl.ds(pl.multiple_of(y * cy2, cy2), cy2)]

        def direct(x, y, ident, to):
            return pltpu.make_async_remote_copy(
                src_ref=place(x, y), dst_ref=place(x, y),
                send_sem=g_send.at[turn, to], recv_sem=g_recv.at[turn, ident],
                device_id=(to // half, 2 * lax.rem(to, half) + parity), device_id_type=MESH,
            )

        def onward(x, y, ident):
            return pltpu.make_async_remote_copy(
                src_ref=place(x, y), dst_ref=place(x, y),
                send_sem=h_send.at[turn, ident], recv_sem=h_recv.at[turn, ident],
                device_id=(mx, partner), device_id_type=MESH,
            )

        def spot(ident, par):
            return ident // half, 2 * lax.rem(ident, half) + par

        def start(j):
            direct(mx, my, mine, lax.rem(mine + 1 + j, many)).start()

        loop(many - 1, start)
        onward(mx, my, mine).start()

        def pass_on(j):
            ident = lax.rem(mine + many - 1 - j, many)
            x, y = spot(ident, parity)
            direct(x, y, ident, ident).wait_recv()
            onward(x, y, ident).start()

        loop(many - 1, pass_on)

        def other(ident):
            x, y = spot(ident, 1 - parity)
            onward(x, y, ident).wait_recv()

        loop(many, other)

        def finish():
            def done(j):
                ident = lax.rem(mine + 1 + j, many)
                direct(mx, my, mine, ident).wait_send()
                x, y = spot(ident, parity)
                onward(x, y, ident).wait_send()

            loop(many - 1, done)
            onward(mx, my, mine).wait_send()

        sizes = [(cx2 * nx, cy2 * ny)]
        for _ in range(2):
            sizes.append((sizes[-1][0] // 2, sizes[-1][1] // 2))
        (x2, y2), (x3, y3), (x4, y4) = sizes

        ghosts(f2, x2)
        sweep_twice_from_zero(f2, v2a, 1, x2, 0.25**2, 4)
        ghosts(v2a, x2)

        def put3(i, value):
            f3[1 + i] = value

        restricted(v2a, f2, tmp, 1, x2, (0, y2), 0.25**2, put3)
        ghosts(f3, x3)
        sweep_twice_from_zero(f3, v3a, 1, x3, 0.25**3, 4)
        ghosts(v3a, x3)

        def put4(i, value):
            f4[1 + i] = value

        restricted(v3a, f3, tmp, 1, x3, (0, y3), 0.25**3, put4)
        total = jnp.sum(jnp.sum(f4[pl.ds(1, x4)], axis=0), axis=0, keepdims=True) / (x4 * y4)
        u = jnp.dot(
            jnp.broadcast_to(total, (8, depth)), green[...],
            preferred_element_type=jnp.float32, precision=lax.Precision.HIGHEST,
        )
        v4a[...] = jnp.broadcast_to(u[0:1][None], v4a.shape)
        for src, dst in ((v4a, v4b), (v4b, v4a), (v4a, v4b), (v4b, v4a)):
            sweep(src, f4, dst, 1, x4, 0.25**4, 8)
            ghosts(dst, x4)

        def climb(e, v, rows, width):
            def body(i):
                doubled(e[1 + i], tmp, 0)
                v[pl.ds(1 + 2 * i, 2)] += read_tmp(tmp, 0, 2 * width)[None]

            loop(rows, body)
            ghosts(v, 2 * rows)

        climb(v4a, v3a, x4, y4)
        sweep(v3a, f3, v3b, 1, x3, 0.25**3, 4)
        ghosts(v3b, x3)
        sweep(v3b, f3, v3a, 1, x3, 0.25**3, 4)
        climb(v3a, v2a, x3, y3)
        sweep(v2a, f2, v2b, 1, x2, 0.25**2, 4)
        ghosts(v2b, x2)
        sweep(v2b, f2, v2a, 1, x2, 0.25**2, 4)
        return finish

    ends = []
    for turn in range(cycles):
        last = turn == cycles - 1
        w = 5 if last else 4
        p_in, f1, f2 = (pa, f1a, f2a) if turn % 2 == 0 else (pb, f1b, f2b)
        sweep(p_in, s, t0, PAD - (w - 1), bx + 2 * (w - 1), 1.0, 2)
        sweep(t0, s, t1, PAD - (w - 2), bx + 2 * (w - 2), 1.0, 2)

        def put1(i, value):
            f1[PAD + i, PAD : PAD + cy1] = value

        restricted(t1, s, tmp, PAD, bx, (PAD, by), 1.0, put1)
        arrive(halo(f1, (cx1, cy1), 5, 2 + 2 * turn))
        sweep_twice_from_zero(f1, v1a, PAD - 4, cx1 + 8, 0.25, 2)

        def put2(i, value):
            f2[1 + mx * cx2 + i, pl.ds(pl.multiple_of(my * cy2, cy2), cy2)] = value

        restricted(v1a, f1, tmp, PAD, cx1, (PAD, cy1), 0.25, put2)
        ends.append(solve_2(f2, turn))

        x2, y2 = cx2 * nx, cy2 * ny

        def down_to_1(i):
            q = lax.rem(mx * cx2 + i - 2 + x2, x2)
            doubled(v2a[1 + q], tmp, PAD)
            for h in range(tmp.shape[0]):
                tmp[h, 0:PAD] = tmp[h, 2 * y2 : 2 * y2 + PAD]
                tmp[h, 2 * y2 + PAD : 2 * y2 + 2 * PAD] = tmp[h, PAD : 2 * PAD]
            e = read_tmp(tmp, pl.multiple_of(my * cy1, PAD), cy1 + 2 * PAD)
            v1a[pl.ds(PAD - 4 + 2 * i, 2)] += e[None]

        loop(cx2 + 4, down_to_1)
        sweep(v1a, f1, v1b, PAD - 3, cx1 + 6, 0.25, 2)
        sweep(v1b, f1, v1a, PAD - 2, cx1 + 4, 0.25, 2)

        reach = 2 if last else 1

        def down_to_0(i):
            doubled(v1a[PAD - reach + i], tmp, 0)
            t1[pl.ds(PAD - 2 * reach + 2 * i, 2)] += read_tmp(tmp, PAD, by + 2 * PAD)[None]

        loop(cx1 + 2 * reach, down_to_0)
        sweep(t1, s, t0, PAD - (w - 3), bx + 2 * (w - 3), 1.0, 2)
        if last:
            sweep(t0, s, t1, PAD - 1, bx + 2, 1.0, 2)
        else:
            following = pb if turn % 2 == 0 else pa
            sweep(t0, s, following, PAD, bx, 1.0, 2, (PAD, PAD + by))
            arrive(halo(following, (bx, by), 5, 3 + 2 * turn))

    store_p = pltpu.make_async_copy(t1.at[pl.ds(PAD, bx), pl.ds(PAD, by)], out_p, local_sem.at[0])
    store_p.start()

    def last_residual(i):
        r = residual_rows(t1, s, PAD + 2 * i, 2, 1.0)
        res[pl.ds(2 * i, 2)] = r[:, PAD : PAD + by]

    loop(bx // 2, last_residual)
    store_r = pltpu.make_async_copy(res, out_r, local_sem.at[1])
    store_r.start()
    for copy in sends:
        copy.wait_send()
    for end in ends:
        end()
    store_p.wait()
    store_r.wait()


def on_device(nx, ny, forces, pressure_prev):
    bx, by, depth = pressure_prev.shape
    cycles = 2
    n = nx * ny
    f32 = jnp.float32

    def vmem(*shape):
        return pltpu.VMEM(shape + (depth,), f32)

    p0 = (bx + 2 * PAD, by + 2 * PAD)
    p1 = (bx // 2 + 2 * PAD, by // 2 + 2 * PAD)
    p2, p3, p4 = ((nx * bx // k + 2, ny * by // k) for k in (4, 8, 16))
    many = n // 2
    sem = pltpu.SemaphoreType.DMA
    scratch = (
        [vmem(bx + 1, by), vmem(bx, by + PAD), vmem(bx, by)]
        + [vmem(*p0)] * 5
        + [vmem(bx, by)]
        + [vmem(*p1)] * 4
        + [vmem(*p2)] * 4
        + [vmem(*p3)] * 3
        + [vmem(*p4)] * 3
        + [vmem(depth)]
        + [pltpu.VMEM((depth // 128, max(2 * p2[1], 2 * p1[1]) + 2 * PAD, 128), f32)]
        + [sem((4,)), sem((2,)), sem((2,))]
        + [sem((2 + 2 * cycles, 8))] * 2
        + [sem((cycles, many))] * 4
    )
    shape = jax.ShapeDtypeStruct((bx, by, depth), f32)
    anyspace = pl.BlockSpec(memory_space=pl.ANY)
    return pl.pallas_call(
        functools.partial(kernel, nx, ny, cycles),
        out_shape=(shape, shape),
        in_specs=[anyspace] * 2,
        out_specs=(anyspace, anyspace),
        scratch_shapes=scratch,
        compiler_params=pltpu.CompilerParams(
            collective_id=0, has_side_effects=True, vmem_limit_bytes=48 * 1024 * 1024
        ),
    )(forces, pressure_prev)


def solution(mesh):
    return jax.shard_map(
        functools.partial(on_device, mesh.shape["gx"], mesh.shape["gy"]),
        mesh=mesh,
        in_specs=(P(None, "gx", "gy", None), P("gx", "gy", None)),
        out_specs=(P("gx", "gy", None), P("gx", "gy", None)),
        check_vma=False,
    )
```

```python
import functools

import jax
import jax.numpy as jnp
from jax import lax
from jax.experimental import pallas as pl
from jax.experimental.pallas import tpu as pltpu
from jax.sharding import PartitionSpec as P

OMEGA = 0.8
PAD = 8
MESH = pl.DeviceIdType.MESH


def loop(count, body):
    def step(i, carry):
        body(i)
        return carry

    lax.fori_loop(0, count, step, 0)


def vertical(c):
    depth = c.shape[-1]
    axis = c.ndim - 1
    lane = lax.broadcasted_iota(jnp.int32, c.shape, axis)
    below = jnp.where(lane == 0, 0.0, pltpu.roll(c, 1, axis))
    above = jnp.where(lane == depth - 1, 0.0, pltpu.roll(c, depth - 1, axis))
    return below + above


def parts(ref, row, count):
    block = ref[pl.ds(row - 1, count + 2)]
    c = block[1:-1]
    width = c.shape[1]
    lateral = (block[:-2] + block[2:]) + (pltpu.roll(c, 1, 1) + pltpu.roll(c, width - 1, 1))
    return c, lateral, vertical(c)


def sweep(src, f, dst, row, rows, weight, unit, cols=None):
    k = OMEGA / (4.0 * weight + 2.0)

    def body(i):
        r = row + i * unit
        c, lateral, up = parts(src, r, unit)
        new = (1.0 - OMEGA) * c + k * (weight * lateral + up + f[pl.ds(r, unit)])
        if cols is None:
            dst[pl.ds(r, unit)] = new
        else:
            dst[pl.ds(r, unit), cols[0] : cols[1]] = new[:, cols[0] : cols[1]]

    loop(rows // unit, body)


def sweep_twice_from_zero(f, dst, row, rows, weight, unit):
    k = OMEGA / (4.0 * weight + 2.0)

    def body(i):
        r = row + i * unit
        c, lateral, up = parts(f, r, unit)
        dst[pl.ds(r, unit)] = k * ((2.0 - OMEGA) * c + k * (weight * lateral + up))

    loop(rows // unit, body)


def residual_rows(v, f, r, count, weight):
    c, lateral, up = parts(v, r, count)
    return f[pl.ds(r, count)] - ((4.0 * weight + 2.0) * c - weight * lateral - up)


def restricted(v, f, tmp, row, rows, cols, weight, put):
    start, count = cols
    depth = v.shape[-1]

    def body(i):
        r = residual_rows(v, f, row + 2 * i, 2, weight)
        both = r[0] + r[1]
        width = both.shape[0]
        halves = []
        for h in range(depth // 128):
            tmp[h, 0:width] = both[:, h * 128 : (h + 1) * 128]
            halves.append(
                tmp[h, pl.ds(start, count // 2, 2)] + tmp[h, pl.ds(start + 1, count // 2, 2)]
            )
        put(i, 0.25 * jnp.concatenate(halves, axis=1))

    loop(rows // 2, body)


def doubled(e, tmp, start):
    width, depth = e.shape
    for h in range(depth // 128):
        piece = e[:, h * 128 : (h + 1) * 128]
        tmp[h, pl.ds(start, width, 2)] = piece
        tmp[h, pl.ds(start + 1, width, 2)] = piece


def read_tmp(tmp, start, width):
    return jnp.concatenate([tmp[h, pl.ds(start, width)] for h in range(tmp.shape[0])], axis=1)


def ghosts(v, rows):
    v[0] = v[rows]
    v[rows + 1] = v[1]


def kernel(
    nx, ny, cycles,
    forces, pressure, out_p, out_r,
    fx, fy, fz, s, pa, pb, t0, t1, res,
    f1a, f1b, v1a, v1b, f2a, f2b, v2a, v2b, f3, v3a, v3b, f4, v4a, v4b, green, tmp,
    local_sem, plane_send, plane_recv, halo_send, halo_recv,
    g_send, g_recv, h_send, h_recv,
):
    mx, my = lax.axis_index("gx"), lax.axis_index("gy")
    n = nx * ny
    me = mx * ny + my
    bx, by, depth = pressure.shape
    cx1, cy1 = bx // 2, by // 2
    cx2, cy2 = bx // 4, by // 4

    loads = [
        pltpu.make_async_copy(forces.at[0], fx.at[pl.ds(1, bx)], local_sem.at[0]),
        pltpu.make_async_copy(forces.at[1], fy.at[:, pl.ds(PAD, by)], local_sem.at[1]),
        pltpu.make_async_copy(pressure, pa.at[pl.ds(PAD, bx), pl.ds(PAD, by)], local_sem.at[2]),
        pltpu.make_async_copy(forces.at[2], fz, local_sem.at[3]),
    ]
    for load in loads:
        load.start()

    barrier = pltpu.get_barrier_semaphore()

    def greet(j):
        other = lax.rem(me + 1 + j, n)
        pl.semaphore_signal(barrier, inc=1, device_id=(other // ny, lax.rem(other, ny)), device_id_type=MESH)

    loop(n - 1, greet)

    row_i = lax.broadcasted_iota(jnp.int32, (depth, depth), 0).astype(jnp.float32)
    col_i = lax.broadcasted_iota(jnp.int32, (depth, depth), 1).astype(jnp.float32)
    green[...] = (jnp.minimum(row_i, col_i) + 1.0) * (depth - jnp.maximum(row_i, col_i)) / (depth + 1.0)

    pl.semaphore_wait(barrier, n - 1)

    sends = []

    def halo(ref, size, width, slot):
        sx, sy = size
        k = min(width, PAD)

        def strip(d, rows, cols, step):
            dx, dy = step
            copy = pltpu.make_async_remote_copy(
                src_ref=ref.at[rows[0], cols[0]],
                dst_ref=ref.at[rows[1], cols[1]],
                send_sem=halo_send.at[slot, d],
                recv_sem=halo_recv.at[slot, d],
                device_id=(lax.rem(mx + dx + nx, nx), lax.rem(my + dy + ny, ny)),
                device_id_type=MESH,
            )
            copy.start()
            sends.append(copy)
            return copy

        def rows_for(dx, w):
            if dx == 1:
                return pl.ds(PAD + sx - w, w), pl.ds(PAD - w, w)
            return pl.ds(PAD, w), pl.ds(PAD + sx, w)

        rows = (pl.ds(PAD, sx), pl.ds(PAD, sx))
        cols = (pl.ds(PAD, sy), pl.ds(PAD, sy))
        low, high = pl.ds(PAD - k, k), pl.ds(PAD + sy, k)
        beside = [
            strip(0, rows, (pl.ds(PAD + sy - k, k), low), (0, 1)),
            strip(1, rows, (pl.ds(PAD, k), high), (0, -1)),
        ]
        late = [
            strip(2, rows_for(1, width), cols, (1, 0)),
            strip(3, rows_for(-1, width), cols, (-1, 0)),
        ]

        def corners():
            for copy in beside:
                copy.wait_recv()
            for d, (dx, side) in enumerate(((1, low), (1, high), (-1, low), (-1, high))):
                late.append(strip(4 + d, rows_for(dx, width - 1), (side, side), (dx, 0)))
            return late

        return corners

    def arrive(copies):
        for copy in copies:
            copy.wait_recv()

    right, above = lax.rem(mx + 1, nx), lax.rem(my + 1, ny)
    loads[0].wait()
    plane_x = pltpu.make_async_remote_copy(
        src_ref=fx.at[pl.ds(bx, 1)], dst_ref=fx.at[pl.ds(0, 1)],
        send_sem=plane_send.at[0], recv_sem=plane_recv.at[0],
        device_id=(right, my), device_id_type=MESH,
    )
    plane_x.start()
    loads[1].wait()
    plane_y = pltpu.make_async_remote_copy(
        src_ref=fy.at[:, pl.ds(PAD + by - 1, 1)], dst_ref=fy.at[:, pl.ds(PAD - 1, 1)],
        send_sem=plane_send.at[1], recv_sem=plane_recv.at[1],
        device_id=(mx, above), device_id_type=MESH,
    )
    plane_y.start()
    sends.extend([plane_x, plane_y])
    loads[2].wait()
    coming_p = halo(pa, (bx, by), 4, 0)
    loads[3].wait()
    plane_x.wait_recv()
    plane_y.wait_recv()

    def make_source(i):
        r = 2 * i
        x = fx[pl.ds(r, 3)]
        y = fy[pl.ds(r, 2)]
        z = fz[pl.ds(r, 2)]
        lane = lax.broadcasted_iota(jnp.int32, z.shape, 2)
        behind_z = jnp.where(lane == 0, 0.0, pltpu.roll(z, 1, 2))
        behind_y = pltpu.roll(y, 1, 1)[:, PAD:]
        s[pl.ds(PAD + r, 2), PAD : PAD + by] = (
            (x[:-1] - x[1:]) + (behind_y - y[:, PAD:]) + (behind_z - z)
        )

    loop(bx // 2, make_source)
    coming_s = halo(s, (bx, by), 4, 1)
    coming = coming_p() + coming_s()

    half = ny // 2
    many = nx * half
    parity = lax.rem(my, 2)
    partner = my + 1 - 2 * parity
    mine = mx * half + my // 2

    def solve_2(f2, turn):
        def place(x, y):
            return f2.at[pl.ds(1 + x * cx2, cx2), pl.ds(pl.multiple_of(y * cy2, cy2), cy2)]

        def direct(x, y, ident, to):
            return pltpu.make_async_remote_copy(
                src_ref=place(x, y), dst_ref=place(x, y),
                send_sem=g_send.at[turn, to], recv_sem=g_recv.at[turn, ident],
                device_id=(to // half, 2 * lax.rem(to, half) + parity), device_id_type=MESH,
            )

        def onward(x, y, ident):
            return pltpu.make_async_remote_copy(
                src_ref=place(x, y), dst_ref=place(x, y),
                send_sem=h_send.at[turn, ident], recv_sem=h_recv.at[turn, ident],
                device_id=(mx, partner), device_id_type=MESH,
            )

        def spot(ident, par):
            return ident // half, 2 * lax.rem(ident, half) + par

        def start(j):
            direct(mx, my, mine, lax.rem(mine + 1 + j, many)).start()

        loop(many - 1, start)
        onward(mx, my, mine).start()

        def pass_on(j):
            ident = lax.rem(mine + many - 1 - j, many)
            x, y = spot(ident, parity)
            direct(x, y, ident, ident).wait_recv()
            onward(x, y, ident).start()

        loop(many - 1, pass_on)

        def other(ident):
            x, y = spot(ident, 1 - parity)
            onward(x, y, ident).wait_recv()

        loop(many, other)

        def finish():
            def done(j):
                ident = lax.rem(mine + 1 + j, many)
                direct(mx, my, mine, ident).wait_send()
                x, y = spot(ident, parity)
                onward(x, y, ident).wait_send()

            loop(many - 1, done)
            onward(mx, my, mine).wait_send()

        sizes = [(cx2 * nx, cy2 * ny)]
        for _ in range(2):
            sizes.append((sizes[-1][0] // 2, sizes[-1][1] // 2))
        (x2, y2), (x3, y3), (x4, y4) = sizes

        ghosts(f2, x2)
        sweep_twice_from_zero(f2, v2a, 1, x2, 0.25**2, 4)
        ghosts(v2a, x2)

        def put3(i, value):
            f3[1 + i] = value

        restricted(v2a, f2, tmp, 1, x2, (0, y2), 0.25**2, put3)
        ghosts(f3, x3)
        sweep_twice_from_zero(f3, v3a, 1, x3, 0.25**3, 8)
        ghosts(v3a, x3)

        def put4(i, value):
            f4[1 + i] = value

        restricted(v3a, f3, tmp, 1, x3, (0, y3), 0.25**3, put4)
        total = jnp.sum(jnp.sum(f4[pl.ds(1, x4)], axis=0), axis=0, keepdims=True) / (x4 * y4)
        u = jnp.dot(
            jnp.broadcast_to(total, (8, depth)), green[...],
            preferred_element_type=jnp.float32, precision=lax.Precision.HIGHEST,
        )
        v4a[...] = jnp.broadcast_to(u[0:1][None], v4a.shape)
        for src, dst in ((v4a, v4b), (v4b, v4a), (v4a, v4b), (v4b, v4a)):
            sweep(src, f4, dst, 1, x4, 0.25**4, 8)
            ghosts(dst, x4)

        def climb(e, v, rows, width):
            def body(i):
                doubled(e[1 + i], tmp, 0)
                v[pl.ds(1 + 2 * i, 2)] += read_tmp(tmp, 0, 2 * width)[None]

            loop(rows, body)
            ghosts(v, 2 * rows)

        climb(v4a, v3a, x4, y4)
        sweep(v3a, f3, v3b, 1, x3, 0.25**3, 8)
        ghosts(v3b, x3)
        sweep(v3b, f3, v3a, 1, x3, 0.25**3, 8)
        climb(v3a, v2a, x3, y3)
        sweep(v2a, f2, v2b, 1, x2, 0.25**2, 4)
        ghosts(v2b, x2)
        sweep(v2b, f2, v2a, 1, x2, 0.25**2, 4)
        return finish

    ends = []
    for turn in range(cycles):
        last = turn == cycles - 1
        w = 5 if last else 4
        p_in, f1, f2 = (pa, f1a, f2a) if turn % 2 == 0 else (pb, f1b, f2b)
        inner = 1 + w % 2
        sweep(p_in, s, t0, PAD + inner, bx - 2 * inner, 1.0, 2)
        sweep(t0, s, t1, PAD + inner + 1, bx - 2 * inner - 2, 1.0, 2)
        arrive(coming)
        for src, dst, reach, off in ((p_in, t0, w - 1, inner), (t0, t1, w - 2, inner + 1)):
            sweep(src, s, dst, PAD - reach, reach + off, 1.0, 2)
            sweep(src, s, dst, PAD + bx - off, reach + off, 1.0, 2)

        def put1(i, value):
            f1[PAD + i, PAD : PAD + cy1] = value

        restricted(t1, s, tmp, PAD, bx, (PAD, by), 1.0, put1)
        coming = halo(f1, (cx1, cy1), 5, 2 + 2 * turn)()
        sweep_twice_from_zero(f1, v1a, PAD + 2, cx1 - 4, 0.25, 2)
        arrive(coming)
        sweep_twice_from_zero(f1, v1a, PAD - 4, 6, 0.25, 2)
        sweep_twice_from_zero(f1, v1a, PAD + cx1 - 2, 6, 0.25, 2)

        def put2(i, value):
            f2[1 + mx * cx2 + i, pl.ds(pl.multiple_of(my * cy2, cy2), cy2)] = value

        restricted(v1a, f1, tmp, PAD, cx1, (PAD, cy1), 0.25, put2)
        ends.append(solve_2(f2, turn))

        x2, y2 = cx2 * nx, cy2 * ny

        def down_to_1(i):
            q = lax.rem(mx * cx2 + i - 2 + x2, x2)
            doubled(v2a[1 + q], tmp, PAD)
            for h in range(tmp.shape[0]):
                tmp[h, 0:PAD] = tmp[h, 2 * y2 : 2 * y2 + PAD]
                tmp[h, 2 * y2 + PAD : 2 * y2 + 2 * PAD] = tmp[h, PAD : 2 * PAD]
            e = read_tmp(tmp, pl.multiple_of(my * cy1, PAD), cy1 + 2 * PAD)
            v1a[pl.ds(PAD - 4 + 2 * i, 2)] += e[None]

        loop(cx2 + 4, down_to_1)
        sweep(v1a, f1, v1b, PAD - 3, cx1 + 6, 0.25, 2)
        sweep(v1b, f1, v1a, PAD - 2, cx1 + 4, 0.25, 2)

        reach = 2 if last else 1

        def down_to_0(i):
            doubled(v1a[PAD - reach + i], tmp, 0)
            t1[pl.ds(PAD - 2 * reach + 2 * i, 2)] += read_tmp(tmp, PAD, by + 2 * PAD)[None]

        loop(cx1 + 2 * reach, down_to_0)
        sweep(t1, s, t0, PAD - (w - 3), bx + 2 * (w - 3), 1.0, 2)
        if last:
            sweep(t0, s, t1, PAD - 1, bx + 2, 1.0, 2)
        else:
            following = pb if turn % 2 == 0 else pa
            sweep(t0, s, following, PAD, bx, 1.0, 2, (PAD, PAD + by))
            coming = halo(following, (bx, by), 5, 3 + 2 * turn)()

    store_p = pltpu.make_async_copy(t1.at[pl.ds(PAD, bx), pl.ds(PAD, by)], out_p, local_sem.at[0])
    store_p.start()

    def last_residual(i):
        r = residual_rows(t1, s, PAD + 2 * i, 2, 1.0)
        res[pl.ds(2 * i, 2)] = r[:, PAD : PAD + by]

    loop(bx // 2, last_residual)
    store_r = pltpu.make_async_copy(res, out_r, local_sem.at[1])
    store_r.start()
    for copy in sends:
        copy.wait_send()
    for end in ends:
        end()
    store_p.wait()
    store_r.wait()


def on_device(nx, ny, forces, pressure_prev):
    bx, by, depth = pressure_prev.shape
    cycles = 2
    n = nx * ny
    f32 = jnp.float32

    def vmem(*shape):
        return pltpu.VMEM(shape + (depth,), f32)

    p0 = (bx + 2 * PAD, by + 2 * PAD)
    p1 = (bx // 2 + 2 * PAD, by // 2 + 2 * PAD)
    p2, p3, p4 = ((nx * bx // k + 2, ny * by // k) for k in (4, 8, 16))
    many = n // 2
    sem = pltpu.SemaphoreType.DMA
    scratch = (
        [vmem(bx + 1, by), vmem(bx, by + PAD), vmem(bx, by)]
        + [vmem(*p0)] * 5
        + [vmem(bx, by)]
        + [vmem(*p1)] * 4
        + [vmem(*p2)] * 4
        + [vmem(*p3)] * 3
        + [vmem(*p4)] * 3
        + [vmem(depth)]
        + [pltpu.VMEM((depth // 128, max(2 * p2[1], 2 * p1[1]) + 2 * PAD, 128), f32)]
        + [sem((4,)), sem((2,)), sem((2,))]
        + [sem((2 + 2 * cycles, 8))] * 2
        + [sem((cycles, many))] * 4
    )
    shape = jax.ShapeDtypeStruct((bx, by, depth), f32)
    anyspace = pl.BlockSpec(memory_space=pl.ANY)
    return pl.pallas_call(
        functools.partial(kernel, nx, ny, cycles),
        out_shape=(shape, shape),
        in_specs=[anyspace] * 2,
        out_specs=(anyspace, anyspace),
        scratch_shapes=scratch,
        compiler_params=pltpu.CompilerParams(
            collective_id=0, has_side_effects=True, vmem_limit_bytes=48 * 1024 * 1024
        ),
    )(forces, pressure_prev)


def solution(mesh):
    return jax.shard_map(
        functools.partial(on_device, mesh.shape["gx"], mesh.shape["gy"]),
        mesh=mesh,
        in_specs=(P(None, "gx", "gy", None), P("gx", "gy", None)),
        out_specs=(P("gx", "gy", None), P("gx", "gy", None)),
        check_vma=False,
    )
```
